512 devices in a mesh: gx: 16 (over z_lo, core), gy: 32 (over x, z_hi, y).
Axes of the slice: x: 4, y: 4, z: 16 (z_hi: 2, z_lo: 8; z = z_hi * 8 + z_lo), core: 2. Of those that a mesh axis runs over, the one named last changes fastest.
Arguments:
- green_ops: bfloat16 [16, 32, 2, 1024, 1024], P('gx', 'gy'), may hold values from -0.125 to 0.125
- cell_map: int32 [16, 32, 1024], P('gx', 'gy'), may hold values from 0 to 2
- dipole_site: int32 [16, 32, 128], P('gx', 'gy'), may hold values from 0 to 1023
- dipole_amp: float32 [16, 32, 2, 128], P('gx', 'gy'), may hold values from -32 to 32
- contrast: float32 [3, 2], replicated, may hold values from 0.3 to 1
Outputs:
- traces: bfloat16 [16, 32, 1024, 2, 128], P('gx', 'gy')
The draws below stay inside these ranges and needn't reach their ends.
All inputs are finite; a program needn't handle non-finite values.
Results may differ from the reference program's by a relative error of at most 0.0069.
Values may be sent and summed in bfloat16 or wider, within the bound.
No kernel may reach another device: no remote copies, remote signals or barrier semaphores. Data moves between devices by JAX's collectives and lax.ppermute only.
A program may use at most 64 MiB of HBM per device.

```python
import jax
import jax.numpy as jnp
from jax import lax

FACE = 512
NB = 64
MB = 2
STEPS = 4
CLASSES = 3
SUBX = 16
SUBY = 32


def plant(values, own_key, smallest, largest):
    index_at = [jax.random.randint(jax.random.fold_in(own_key, axis), (), 0, length) for axis, length in enumerate(values.shape)]
    main_axis = values.shape.index(max(values.shape))
    beside = index_at[:main_axis] + [(index_at[main_axis] + 1) % values.shape[main_axis]] + index_at[main_axis + 1:]
    return values.at[tuple(index_at)].set(smallest).at[tuple(beside)].set(largest)


def levels(stream_key, dims, split, least, high):
    factor_of = 1.0
    for position, shards_of in split:
        steps = jax.random.uniform(jax.random.fold_in(jax.random.fold_in(stream_key, 6), position), (shards_of,), jnp.float32, least / len(split), high / len(split))
        factor_of = factor_of * jnp.repeat(jnp.exp(steps), dims[position] // shards_of).reshape((-1,) + (1,) * (len(dims) - 1 - position))
    return factor_of


def gaussian(stream_key, extent, deviation, reach, cuts=(), dtype=jnp.bfloat16):
    gain = levels(stream_key, extent, cuts, -0.22, 0.18) if cuts else 1.0
    entries = jax.random.normal(stream_key, extent, jnp.float32) * deviation * gain
    return jnp.minimum(jnp.maximum(entries, -reach), reach).astype(dtype)


def setup_inputs(seed: int = 0) -> dict:
    arg_keys = jax.random.split(jax.random.key(seed), 6)
    green_ops = gaussian(arg_keys[0], (SUBX, SUBY, 2, 2 * FACE, 2 * FACE), (4 * FACE) ** -0.5, 0.125, ((0, 16), (1, 32)))
    cell_map = plant(jax.random.randint(arg_keys[1], (SUBX, SUBY, 2 * FACE), 0, CLASSES), jax.random.fold_in(arg_keys[1], 1), 0, CLASSES - 1).astype(jnp.int32)
    dipole_site = plant(jax.random.randint(arg_keys[2], (SUBX, SUBY, MB * NB), 0, 2 * FACE), jax.random.fold_in(arg_keys[2], 1), 0, (2 * FACE) - 1).astype(jnp.int32)
    dipole_amp = jnp.clip(jax.random.uniform(arg_keys[3], (SUBX, SUBY, 2, MB * NB), jnp.float32, -32.0, 32.0) * levels(arg_keys[3], (SUBX, SUBY, 2, MB * NB), ((0, 16), (1, 32)), -0.4, 0.0), -32.0, 32.0)
    contrast = jnp.clip(jax.random.uniform(arg_keys[4], (CLASSES, 2), jnp.float32, 0.3, 1.0), 0.3, 1.0)
    return {"green_ops": green_ops, "cell_map": cell_map, "dipole_site": dipole_site, "dipole_amp": dipole_amp, "contrast": contrast}


def apply_row(pair):
    ops_row, excited_row = pair
    ops_wide = ops_row.astype(jnp.float32)
    data_wide = excited_row.astype(jnp.float32)
    product = jnp.einsum('jspq,jqrc->jsprc', ops_wide, data_wide, precision=lax.Precision.HIGHEST)
    real_out = product[:, 0, :, 0] - product[:, 1, :, 1]
    imag_out = product[:, 0, :, 1] + product[:, 1, :, 0]
    return jnp.stack([real_out, imag_out], axis=2).astype(jnp.bfloat16)


def reference(green_ops, cell_map, dipole_site, dipole_amp, contrast):
    trace_rows = 2 * FACE
    columns = MB * NB
    one_hot = (lax.broadcasted_iota(jnp.int32, (SUBX, SUBY, trace_rows, columns), 2) == dipole_site[:, :, None, :]).astype(jnp.float32)
    source = one_hot[:, :, :, None, :] * dipole_amp[:, :, None, :, :]
    factor = contrast[cell_map]
    real_factor = factor[..., 0][..., None]
    imag_factor = factor[..., 1][..., None]
    batch_index = lax.broadcasted_iota(jnp.int32, (columns,), 0) // NB
    traces = jnp.zeros((SUBX, SUBY, trace_rows, 2, columns), jnp.bfloat16)
    for turn_index in range(STEPS):
        east_trace = traces[:, :, :FACE]
        north_trace = traces[:, :, FACE:]
        west_trace = jnp.concatenate([jnp.zeros_like(east_trace[:1]), east_trace[:-1]], axis=0)
        south_trace = jnp.concatenate([jnp.zeros_like(north_trace[:, :1]), north_trace[:, :-1]], axis=1)
        incoming = jnp.concatenate([west_trace, south_trace], axis=2).astype(jnp.float32)
        real_in = real_factor * incoming[..., 0, :] - imag_factor * incoming[..., 1, :] + source[..., 0, :]
        imag_in = real_factor * incoming[..., 1, :] + imag_factor * incoming[..., 0, :] + source[..., 1, :]
        excited = jnp.stack([real_in, imag_in], axis=3).astype(jnp.bfloat16)
        image = lax.map(apply_row, (green_ops, excited))
        traces = jnp.where(batch_index <= turn_index, image, jnp.zeros_like(image))
    return traces
```

```python
import jax
import jax.numpy as jnp
from jax import lax
from jax.sharding import PartitionSpec as P


NB = 64
BLOCK = 4
PIECES = ((3, 48), (1, 40), (0, 40))


def per_device(green_ops, cell_map, dipole_site, dipole_amp, contrast):
    operator = green_ops[0, 0]
    cells = cell_map[0]
    sites = dipole_site[0, 0]
    amplitude = dipole_amp[0, 0]
    rows = operator.shape[1]
    face = rows // 2
    width = sites.shape[0]
    n_gx = lax.axis_size("gx")
    n_gy = lax.axis_size("gy")
    blocks = n_gy // BLOCK
    lane = lax.axis_index("gy") % BLOCK

    hot = lax.broadcasted_iota(jnp.int32, (width, rows), 1) == sites[:, None]
    source = jnp.where(hot[None], amplitude[:, :, None], 0.0)

    def factor_of(part):
        return jnp.where(
            cells == 0, contrast[0, part], jnp.where(cells == 1, contrast[1, part], contrast[2, part])
        )

    real_factor = factor_of(0)
    imag_factor = factor_of(1)

    def apply(excited):
        live = excited.shape[1]
        flat = excited.reshape(2 * live, rows)
        product = lax.dot_general(
            flat, operator, (((1,), (2,)), ((), ())), preferred_element_type=jnp.float32
        )
        product = product.reshape(2, live, 2, rows)
        real_out = product[0, :, 0] - product[1, :, 1]
        imag_out = product[1, :, 0] + product[0, :, 1]
        return jnp.stack([real_out, imag_out]).astype(jnp.bfloat16)

    def step(west, south):
        incoming = jnp.concatenate([west, south], axis=2).astype(jnp.float32)
        live = incoming.shape[1]
        real_in = real_factor * incoming[0] - imag_factor * incoming[1] + source[0, :live]
        imag_in = real_factor * incoming[1] + imag_factor * incoming[0] + source[1, :live]
        return apply(jnp.stack([real_in, imag_in]).astype(jnp.bfloat16))

    def east_to(traces, lanes):
        pairs = [
            (i * n_gy + j, (i + 1) * n_gy + j)
            for i in range(n_gx - 1)
            for j in range(n_gy)
            if j % BLOCK in lanes
        ]
        return lax.ppermute(traces[:, :, :face], ("gx", "gy"), pairs)

    def north_to(traces, lanes):
        pairs = [(j, j + 1) for j in range(n_gy) if j % BLOCK in lanes]
        return lax.ppermute(traces[:, :, face:], "gy", pairs)

    def cross(traces):
        north = traces[:, :, face:]
        live = north.shape[1]
        at = 0
        pieces = []
        for column, share in PIECES:
            size = share * live // width
            pieces.append((column, north[:, at : at + size]))
            at += size
        moved = []
        for column, piece in pieces:
            if column != BLOCK - 1:
                pairs = [(b * BLOCK + BLOCK - 1, b * BLOCK + column) for b in range(blocks - 1)]
                piece = lax.ppermute(piece, "gy", pairs)
            moved.append((column, piece))
        arrived = []
        for column, piece in moved:
            pairs = [(b * BLOCK + column, (b + 1) * BLOCK) for b in range(blocks - 1)]
            arrived.append(lax.ppermute(piece, "gy", pairs))
        return jnp.concatenate(arrived, axis=1)

    t0 = apply(source.astype(jnp.bfloat16))
    w1 = east_to(t0, (0, 1, 2, 3))
    s1 = north_to(t0, (0, 1, 2))
    x1 = cross(t0)

    t1 = step(w1, s1)
    w2 = east_to(t1, (1, 2, 3))
    s2 = north_to(t1, (1, 2))
    x2 = cross(t1)

    t2 = step(jnp.where(lane == 0, w1, w2), jnp.where(lane == 0, x1, s2))
    w3 = east_to(t2, (0, 2, 3))
    s3 = north_to(t2, (0, 2))
    x3 = cross(t2[:, :NB])

    t3 = step(jnp.where(lane == 1, w2, w3), jnp.where(lane == 0, x2, s3))
    w4 = east_to(t3[:, :NB], (0, 1))
    s4 = north_to(t3[:, :NB], (0, 1))

    t4 = step(jnp.where(lane == 2, w3[:, :NB], w4), jnp.where(lane == 0, x3, s4))

    first = jnp.where(lane == 3, t3[:, :NB], t4)
    second = jnp.where(lane >= 2, t2[:, NB:], t3[:, NB:])
    traces = jnp.concatenate([first, second], axis=1)
    return traces.transpose(2, 0, 1)[None, None]


def solution(mesh):
    placed = (
        P("gx", "gy", None, None, None),
        P("gx", "gy", None),
        P("gx", "gy", None),
        P("gx", "gy", None, None),
        P(),
    )
    return jax.shard_map(
        per_device,
        mesh=mesh,
        in_specs=placed,
        out_specs=P("gx", "gy", None, None, None),
        check_vma=False,
    )
```

```python
import jax
import jax.numpy as jnp
from jax import lax
from jax.experimental import pallas as pl
from jax.sharding import PartitionSpec as P


NB = 64
BLOCK = 4
PIECES = ((3, 48), (1, 40), (2, 40))


def copy_kernel(source_ref, target_ref):
    target_ref[...] = source_ref[...]


def per_device(green_ops, cell_map, dipole_site, dipole_amp, contrast):
    operator = green_ops[0, 0]
    cells = cell_map[0]
    sites = dipole_site[0, 0]
    amplitude = dipole_amp[0, 0]
    rows = operator.shape[1]
    face = rows // 2
    width = sites.shape[0]
    n_gx = lax.axis_size("gx")
    n_gy = lax.axis_size("gy")
    blocks = n_gy // BLOCK
    lane = lax.axis_index("gy") % BLOCK

    hot = lax.broadcasted_iota(jnp.int32, (width, rows), 1) == sites[:, None]
    source = jnp.where(hot[None], amplitude[:, :, None], 0.0)

    classes = lax.broadcasted_iota(jnp.int32, (contrast.shape[0], 1, rows), 0)
    factor = jnp.where(classes == cells[None], contrast[:, :, None], 0.0).sum(axis=0)

    def apply(excited):
        live = excited.shape[1]
        flat = excited.reshape(2 * live, rows)
        product = lax.dot_general(
            flat, operator, (((1,), (2,)), ((), ())), preferred_element_type=jnp.float32
        )
        product = product.reshape(2, live, 2, rows)
        real_out = product[0, :, 0] - product[1, :, 1]
        imag_out = product[1, :, 0] + product[0, :, 1]
        return jnp.stack([real_out, imag_out]).astype(jnp.bfloat16)

    def step(west, south):
        real_factor, imag_factor = factor[0:1], factor[1:2]
        incoming = jnp.concatenate([west, south], axis=2).astype(jnp.float32)
        live = incoming.shape[1]
        real_in = real_factor * incoming[0] - imag_factor * incoming[1] + source[0, :live]
        imag_in = real_factor * incoming[1] + imag_factor * incoming[0] + source[1, :live]
        return apply(jnp.stack([real_in, imag_in]).astype(jnp.bfloat16))

    def east_to(traces, lanes):
        pairs = [
            (i * n_gy + j, (i + 1) * n_gy + j)
            for i in range(n_gx - 1)
            for j in range(n_gy)
            if j % BLOCK in lanes
        ]
        return lax.ppermute(traces[:, :, :face], ("gx", "gy"), pairs)

    def north_to(traces, lanes):
        pairs = [(j, j + 1) for j in range(n_gy) if j % BLOCK in lanes]
        return lax.ppermute(traces[:, :, face:], "gy", pairs)

    def cross(traces):
        north = traces[:, :, face:]
        live = north.shape[1]
        at = 0
        pieces = []
        for column, share in PIECES:
            size = share * live // width
            pieces.append((column, north[:, at : at + size]))
            at += size
        moved = []
        for column, piece in pieces:
            if column != BLOCK - 1:
                pairs = [(b * BLOCK + BLOCK - 1, b * BLOCK + column) for b in range(blocks - 1)]
                piece = lax.ppermute(piece, "gy", pairs)
            moved.append((column, piece))
        arrived = []
        for column, piece in moved:
            pairs = [(b * BLOCK + column, (b + 1) * BLOCK) for b in range(blocks - 1)]
            arrived.append(lax.ppermute(piece, "gy", pairs))
        return jnp.concatenate(arrived, axis=1)

    t0 = apply(source.astype(jnp.bfloat16))
    w1 = east_to(t0, (0, 1, 2, 3))
    s1 = north_to(t0, (0, 1, 2))
    x1 = cross(t0)

    t1 = step(w1, s1)
    w2 = east_to(t1, (1, 2, 3))
    s2 = north_to(t1, (1, 2))
    x2 = cross(t1)

    t2 = step(w2, s2)
    x3 = cross(t2[:, :NB])

    factor = pl.pallas_call(copy_kernel, out_shape=jax.ShapeDtypeStruct(factor.shape, factor.dtype))(factor)
    w1, x1, t2 = lax.optimization_barrier((w1, x1, t2))
    late1 = step(w1, x1)
    w3 = east_to(late1, (0,))
    s3 = north_to(late1, (0,))

    late2 = step(jnp.where(lane == 0, w3, w2), jnp.where(lane == 0, x2, s3))
    after_two = jnp.where(lane >= 2, t2, late2)
    first = after_two[:, :NB]
    w4 = east_to(first, (0, 1, 2, 3))
    s4 = north_to(first, (0, 1, 2))

    t3 = step(w4, jnp.where(lane == 0, x3, s4))
    traces = jnp.concatenate([t3, after_two[:, NB:]], axis=1)
    return traces.transpose(2, 0, 1)[None, None]


def solution(mesh):
    placed = (
        P("gx", "gy", None, None, None),
        P("gx", "gy", None),
        P("gx", "gy", None),
        P("gx", "gy", None, None),
        P(),
    )
    return jax.shard_map(
        per_device,
        mesh=mesh,
        in_specs=placed,
        out_specs=P("gx", "gy", None, None, None),
        check_vma=False,
    )
```

```python
import jax
import jax.numpy as jnp
from jax import lax
from jax.experimental import pallas as pl
from jax.sharding import PartitionSpec as P


NB = 64
BLOCK = 4
PIECES = {1: ((3, 64), (2, 64)), 2: ((3, 64), (2, 64)), 3: ((3, 32), (2, 32))}


def copy_kernel(source_ref, target_ref):
    target_ref[...] = source_ref[...]


def per_device(green_ops, cell_map, dipole_site, dipole_amp, contrast):
    operator = green_ops[0, 0]
    cells = cell_map[0]
    sites = dipole_site[0, 0]
    amplitude = dipole_amp[0, 0]
    rows = operator.shape[1]
    face = rows // 2
    width = sites.shape[0]
    n_gx = lax.axis_size("gx")
    n_gy = lax.axis_size("gy")
    blocks = n_gy // BLOCK
    lane = lax.axis_index("gy") % BLOCK

    hot = lax.broadcasted_iota(jnp.int32, (width, rows), 1) == sites[:, None]
    source = jnp.where(hot[None], amplitude[:, :, None], 0.0)

    classes = lax.broadcasted_iota(jnp.int32, (contrast.shape[0], 1, rows), 0)
    factor = jnp.where(classes == cells[None], contrast[:, :, None], 0.0).sum(axis=0)

    def apply(excited):
        live = excited.shape[1]
        flat = excited.reshape(2 * live, rows)
        product = lax.dot_general(
            flat, operator, (((1,), (2,)), ((), ())), preferred_element_type=jnp.float32
        )
        product = product.reshape(2, live, 2, rows)
        real_out = product[0, :, 0] - product[1, :, 1]
        imag_out = product[1, :, 0] + product[0, :, 1]
        return jnp.stack([real_out, imag_out]).astype(jnp.bfloat16)

    def step(west, south):
        real_factor, imag_factor = factor[0:1], factor[1:2]
        incoming = jnp.concatenate([west, south], axis=2).astype(jnp.float32)
        live = incoming.shape[1]
        real_in = real_factor * incoming[0] - imag_factor * incoming[1] + source[0, :live]
        imag_in = real_factor * incoming[1] + imag_factor * incoming[0] + source[1, :live]
        return apply(jnp.stack([real_in, imag_in]).astype(jnp.bfloat16))

    def east_to(traces, lanes):
        pairs = [
            (i * n_gy + j, (i + 1) * n_gy + j)
            for i in range(n_gx - 1)
            for j in range(n_gy)
            if j % BLOCK in lanes
        ]
        return lax.ppermute(traces[:, :, :face], ("gx", "gy"), pairs)

    def north_to(traces, lanes):
        pairs = [(j, j + 1) for j in range(n_gy) if j % BLOCK in lanes]
        return lax.ppermute(traces[:, :, face:], "gy", pairs)

    def cross(traces, name):
        north = traces[:, :, face:]
        at = 0
        pieces = []
        for column, size in PIECES[int(name[1])]:
            pieces.append((column, north[:, at : at + size]))
            at += size
        moved = []
        for column, piece in pieces:
            if column != BLOCK - 1:
                pairs = [(b * BLOCK + BLOCK - 1, b * BLOCK + column) for b in range(blocks - 1)]
                piece = lax.ppermute(piece, "gy", pairs)
            moved.append((column, piece))
        arrived = []
        for column, piece in moved:
            pairs = [(b * BLOCK + column, (b + 1) * BLOCK) for b in range(blocks - 1)]
            arrived.append(lax.ppermute(piece, "gy", pairs))
        return jnp.concatenate(arrived, axis=1)

    t0 = apply(source.astype(jnp.bfloat16))
    w1 = east_to(t0, (0, 1, 2, 3))
    s1 = north_to(t0, (0, 1, 2))
    x1 = cross(t0, "x1")

    t1 = step(w1, s1)
    w2 = east_to(t1, (1, 2, 3))
    s2 = north_to(t1, (1, 2))
    x2 = cross(t1, "x2")

    t2 = step(w2, s2)
    x3 = cross(t2[:, :NB], "x3")

    factor = pl.pallas_call(
        copy_kernel, out_shape=jax.ShapeDtypeStruct(factor.shape, factor.dtype)
    )(factor)
    w1, x1, t2 = lax.optimization_barrier((w1, x1, t2))
    late1 = step(w1, x1)
    w3 = east_to(late1, (0,))
    s3 = north_to(late1, (0,))

    late2 = step(jnp.where(lane == 0, w3, w2), jnp.where(lane == 0, x2, s3))
    after_two = jnp.where(lane >= 2, t2, late2)
    first = after_two[:, :NB]
    w4 = east_to(first, (0, 1, 2, 3))
    s4 = north_to(first, (0, 1, 2))

    t3 = step(w4, jnp.where(lane == 0, x3, s4))
    traces = jnp.concatenate([t3, after_two[:, NB:]], axis=1)
    return traces.transpose(2, 0, 1)[None, None]


def solution(mesh):
    placed = (
        P("gx", "gy", None, None, None),
        P("gx", "gy", None),
        P("gx", "gy", None),
        P("gx", "gy", None, None),
        P(),
    )
    return jax.shard_map(
        per_device,
        mesh=mesh,
        in_specs=placed,
        out_specs=P("gx", "gy", None, None, None),
        check_vma=False,
    )
```

```python
import jax
import jax.numpy as jnp
from jax import lax
from jax.experimental import pallas as pl
from jax.sharding import PartitionSpec as P


NB = 64
BLOCK = 4
PIECES = {1: ((3, 64), (2, 64)), 2: ((3, 64), (2, 64)), 3: ((3, 32), (2, 32))}


def split_kernel(factor_ref, real_ref, imag_ref):
    real_ref[...] = factor_ref[0:1]
    imag_ref[...] = factor_ref[1:2]


def per_device(green_ops, cell_map, dipole_site, dipole_amp, contrast):
    operator = green_ops[0, 0]
    cells = cell_map[0]
    sites = dipole_site[0, 0]
    amplitude = dipole_amp[0, 0]
    rows = operator.shape[1]
    face = rows // 2
    width = sites.shape[0]
    n_gx = lax.axis_size("gx")
    n_gy = lax.axis_size("gy")
    blocks = n_gy // BLOCK
    lane = lax.axis_index("gy") % BLOCK

    hot = lax.broadcasted_iota(jnp.int32, (width, rows), 1) == sites[:, None]
    source = jnp.where(hot[None], amplitude[:, :, None], 0.0)

    classes = lax.broadcasted_iota(jnp.int32, (contrast.shape[0], 1, rows), 0)
    factor = jnp.where(classes == cells[None], contrast[:, :, None], 0.0).sum(axis=0)
    factor = (factor[0:1], factor[1:2])

    def apply(excited):
        live = excited.shape[1]
        flat = excited.reshape(2 * live, rows)
        product = lax.dot_general(
            flat, operator, (((1,), (2,)), ((), ())), preferred_element_type=jnp.float32
        )
        product = product.reshape(2, live, 2, rows)
        real_out = product[0, :, 0] - product[1, :, 1]
        imag_out = product[1, :, 0] + product[0, :, 1]
        return jnp.stack([real_out, imag_out]).astype(jnp.bfloat16)

    def step(west, south):
        real_factor, imag_factor = factor
        incoming = jnp.concatenate([west, south], axis=2).astype(jnp.float32)
        live = incoming.shape[1]
        real_in = real_factor * incoming[0] - imag_factor * incoming[1] + source[0, :live]
        imag_in = real_factor * incoming[1] + imag_factor * incoming[0] + source[1, :live]
        return apply(jnp.stack([real_in, imag_in]).astype(jnp.bfloat16))

    def east_to(traces, lanes):
        pairs = [
            (i * n_gy + j, (i + 1) * n_gy + j)
            for i in range(n_gx - 1)
            for j in range(n_gy)
            if j % BLOCK in lanes
        ]
        return lax.ppermute(traces[:, :, :face], ("gx", "gy"), pairs)

    def north_to(traces, lanes):
        pairs = [(j, j + 1) for j in range(n_gy) if j % BLOCK in lanes]
        return lax.ppermute(traces[:, :, face:], "gy", pairs)

    def cross(traces, name):
        north = traces[:, :, face:]
        at = 0
        pieces = []
        for column, size in PIECES[int(name[1])]:
            pieces.append((column, north[:, at : at + size]))
            at += size
        moved = []
        for column, piece in pieces:
            if column != BLOCK - 1:
                pairs = [(b * BLOCK + BLOCK - 1, b * BLOCK + column) for b in range(blocks - 1)]
                piece = lax.ppermute(piece, "gy", pairs)
            moved.append((column, piece))
        arrived = []
        for column, piece in moved:
            pairs = [(b * BLOCK + column, (b + 1) * BLOCK) for b in range(blocks - 1)]
            arrived.append(lax.ppermute(piece, "gy", pairs))
        return jnp.concatenate(arrived, axis=1)

    t0 = apply(source.astype(jnp.bfloat16))
    w1 = east_to(t0, (0, 1, 2, 3))
    s1 = north_to(t0, (0, 1, 2))
    x1 = cross(t0, "x1")

    t1 = step(w1, s1)
    w2 = east_to(t1, (1, 2, 3))
    s2 = north_to(t1, (1, 2))
    x2 = cross(t1, "x2")

    t2 = step(w2, s2)
    x3 = cross(t2[:, :NB], "x3")

    part = jax.ShapeDtypeStruct((1, rows), jnp.float32)
    factor = pl.pallas_call(split_kernel, out_shape=(part, part))(jnp.concatenate(factor))
    w1, x1, t2 = lax.optimization_barrier((w1, x1, t2))
    late1 = step(w1, x1)
    w3 = east_to(late1, (0,))
    s3 = north_to(late1, (0,))

    late2 = step(jnp.where(lane == 0, w3, w2), jnp.where(lane == 0, x2, s3))
    after_two = jnp.where(lane >= 2, t2, late2)
    first = after_two[:, :NB]
    w4 = east_to(first, (0, 1, 2, 3))
    s4 = north_to(first, (0, 1, 2))

    t3 = step(w4, jnp.where(lane == 0, x3, s4))
    traces = jnp.concatenate([t3, after_two[:, NB:]], axis=1)
    return traces.transpose(2, 0, 1)[None, None]


def solution(mesh):
    placed = (
        P("gx", "gy", None, None, None),
        P("gx", "gy", None),
        P("gx", "gy", None),
        P("gx", "gy", None, None),
        P(),
    )
    return jax.shard_map(
        per_device,
        mesh=mesh,
        in_specs=placed,
        out_specs=P("gx", "gy", None, None, None),
        check_vma=False,
    )
```
